16 devices in a mesh: cp: 16 (over z, y, x, core).
Axes of the slice: x: 2, y: 2, z: 2, core: 2. Of those that a mesh axis runs over, the one named last changes fastest.
Arguments:
- hidden: bfloat16 [8, 2048, 2048], P(None, 'cp')
- grad_out: bfloat16 [8, 2048, 2048], P(None, 'cp')
- positions: int32 [8, 2048], P(None, 'cp')
- seg_ids: int32 [8, 2048], P(None, 'cp')
- w_q: bfloat16 [2048, 2048], replicated
- w_k: bfloat16 [2048, 256], replicated
- w_v: bfloat16 [2048, 256], replicated
- w_o: bfloat16 [2048, 2048], replicated
- norm_gain: bfloat16 [2048], replicated
Outputs:
- output 1: bfloat16 [8, 2048, 2048], P(None, 'cp')
- output 2: bfloat16 [8, 2048, 2048], P(None, 'cp')
- output 3: float32 [2048, 2048], replicated
- output 4: float32 [2048, 256], replicated
- output 5: float32 [2048, 256], replicated
- output 6: float32 [2048, 2048], replicated
- output 7: float32 [2048], replicated
All inputs are finite; a program needn't handle non-finite values.
Results may differ from the reference program's by a relative error of at most 0.0127539.
Values are sent between devices in bfloat16 or wider.
A program may use at most 1 GiB of HBM per device.

```python
import jax
import jax.numpy as jnp
from jax import lax

BATCH = 8
CHUNK = 64
CP_SIZE = 16
D_MODEL = 2048
HEADS = 16
KV_HEADS = 2
HEAD_DIM = 128
NUM_CUTS = 12

SEQ_LEN = 2 * CP_SIZE * CHUNK
GROUP_SIZE = HEADS // KV_HEADS
NORM_EPS = 1e-5
ROPE_BASE = 500000.0
ATTN_SCALE = HEAD_DIM ** -0.5
NEG_BIG = -1e30


def storage_order(glob_rows):
    blocks = glob_rows.reshape(BATCH, 2 * CP_SIZE, CHUNK)
    front_half = blocks[:, :CP_SIZE]
    back_half = blocks[:, CP_SIZE:][:, ::-1]
    return jnp.stack([front_half, back_half], axis=2).reshape(BATCH, SEQ_LEN)


def draw_layout(layout_key):
    key_start, key_len, key_cut = jax.random.split(layout_key, 3)
    long_start = jax.random.randint(key_start, (BATCH, 1), 0, SEQ_LEN // 4 + 1)
    long_end = long_start + SEQ_LEN // 2 + jax.random.randint(key_len, (BATCH, 1), 0, SEQ_LEN // 4 + 1)
    cut_points = jax.random.randint(key_cut, (BATCH, NUM_CUTS), 1, SEQ_LEN)
    keep_cut = (cut_points <= long_start) | (cut_points >= long_end)
    bounds = jnp.concatenate([jnp.where(keep_cut, cut_points, 0), long_start, long_end], axis=1)
    token_idx = jnp.arange(SEQ_LEN)
    passed = (bounds[:, :, None] <= token_idx[None, None, :]) & (bounds[:, :, None] > 0)
    seg_glob = jnp.sum(passed.astype(jnp.int32), axis=1)
    doc_start = jnp.max(jnp.where(passed, bounds[:, :, None], 0), axis=1)
    pos_glob = token_idx[None, :] - doc_start
    return storage_order(pos_glob.astype(jnp.int32)), storage_order(seg_glob.astype(jnp.int32))


def setup_inputs(seed: int = 0) -> dict:
    root_key = jax.random.key(seed)
    key_list = jax.random.split(root_key, 9)
    positions, seg_ids = draw_layout(key_list[0])
    hidden = jax.random.normal(key_list[1], (BATCH, SEQ_LEN, D_MODEL), jnp.float32)
    grad_out = jax.random.normal(key_list[2], (BATCH, SEQ_LEN, D_MODEL), jnp.float32)
    w_q = jax.random.normal(key_list[3], (D_MODEL, HEADS * HEAD_DIM), jnp.float32) * D_MODEL ** -0.5
    w_k = jax.random.normal(key_list[4], (D_MODEL, KV_HEADS * HEAD_DIM), jnp.float32) * D_MODEL ** -0.5
    w_v = jax.random.normal(key_list[5], (D_MODEL, KV_HEADS * HEAD_DIM), jnp.float32) * D_MODEL ** -0.5
    w_o = jax.random.normal(key_list[6], (HEADS * HEAD_DIM, D_MODEL), jnp.float32) * (HEADS * HEAD_DIM) ** -0.5
    norm_gain = jax.random.uniform(key_list[7], (D_MODEL,), jnp.float32, 0.5, 1.5)
    return {
        'hidden': hidden.astype(jnp.bfloat16),
        'grad_out': grad_out.astype(jnp.bfloat16),
        'positions': positions,
        'seg_ids': seg_ids,
        'w_q': w_q.astype(jnp.bfloat16),
        'w_k': w_k.astype(jnp.bfloat16),
        'w_v': w_v.astype(jnp.bfloat16),
        'w_o': w_o.astype(jnp.bfloat16),
        'norm_gain': norm_gain.astype(jnp.bfloat16),
    }


def global_index():
    chunk_slots = jnp.arange(2 * CP_SIZE)
    owner_rank = chunk_slots // 2
    glob_chunk = jnp.where(chunk_slots % 2 == 0, owner_rank, 2 * CP_SIZE - 1 - owner_rank)
    return (glob_chunk[:, None] * CHUNK + jnp.arange(CHUNK)[None, :]).reshape(SEQ_LEN)


def rms_norm(hidden_f32, gain_f32):
    inv_rms = lax.rsqrt(jnp.mean(hidden_f32 * hidden_f32, axis=-1, keepdims=True) + NORM_EPS)
    return (hidden_f32 * inv_rms * gain_f32).astype(jnp.bfloat16)


def rope_tables(positions):
    inv_freq = ROPE_BASE ** (-jnp.arange(0, HEAD_DIM, 2).astype(jnp.float32) / HEAD_DIM)
    angles = positions.astype(jnp.float32)[..., None] * inv_freq
    angles = jnp.concatenate([angles, angles], axis=-1)
    return jnp.cos(angles), jnp.sin(angles)


def rotate(proj_in, cos_t, sin_t):
    half_dim = proj_in.shape[-1] // 2
    turned = jnp.concatenate([-proj_in[..., half_dim:], proj_in[..., :half_dim]], axis=-1)
    return proj_in * cos_t + turned * sin_t


def attention(queries, keys_all, values_all, seg_ids):
    glob_all = global_index()
    n_blocks = 2 * CP_SIZE * KV_HEADS
    q_blocks = queries.reshape(BATCH, 2 * CP_SIZE, CHUNK, KV_HEADS, GROUP_SIZE, HEAD_DIM).transpose(1, 3, 0, 2, 4, 5).reshape(n_blocks, BATCH, CHUNK, GROUP_SIZE, HEAD_DIM)
    glob_blocks = jnp.repeat(glob_all.reshape(2 * CP_SIZE, CHUNK), KV_HEADS, axis=0)
    seg_blocks = jnp.repeat(seg_ids.reshape(BATCH, 2 * CP_SIZE, CHUNK).transpose(1, 0, 2), KV_HEADS, axis=0)
    head_ids = jnp.tile(jnp.arange(KV_HEADS), 2 * CP_SIZE)
    keys_t = jnp.moveaxis(keys_all, 2, 0)
    values_t = jnp.moveaxis(values_all, 2, 0)

    def block_attend(operands):
        q_blk, glob_q, seg_q, head_id = operands
        scores = jnp.einsum('bqgd,bsd->bgqs', q_blk, keys_t[head_id]) * ATTN_SCALE
        allowed = (seg_q[:, :, None] == seg_ids[:, None, :]) & (glob_q[:, None] >= glob_all[None, :])[None]
        attn_probs = jax.nn.softmax(jnp.where(allowed[:, None], scores, NEG_BIG), axis=-1)
        attn_probs = attn_probs.astype(jnp.bfloat16).astype(jnp.float32)
        return jnp.einsum('bgqs,bsd->bqgd', attn_probs, values_t[head_id])

    out_blocks = lax.map(jax.checkpoint(block_attend), (q_blocks, glob_blocks, seg_blocks, head_ids))
    attn_out = out_blocks.reshape(2 * CP_SIZE, KV_HEADS, BATCH, CHUNK, GROUP_SIZE, HEAD_DIM).transpose(2, 0, 3, 1, 4, 5)
    return attn_out.reshape(BATCH * SEQ_LEN, HEADS * HEAD_DIM).astype(jnp.bfloat16).astype(jnp.float32)


def forward(hidden, positions, seg_ids, wq_f32, wk_f32, wv_f32, wo_f32, gain_f32):
    hidden_f32 = hidden.astype(jnp.float32)
    normed = rms_norm(hidden_f32, gain_f32).astype(jnp.float32).reshape(BATCH * SEQ_LEN, D_MODEL)
    cos_t, sin_t = rope_tables(positions)
    q_lin = jnp.dot(normed, wq_f32, preferred_element_type=jnp.float32).reshape(BATCH, SEQ_LEN, KV_HEADS, GROUP_SIZE, HEAD_DIM)
    queries = rotate(q_lin, cos_t[:, :, None, None], sin_t[:, :, None, None]).astype(jnp.bfloat16).astype(jnp.float32)
    k_lin = jnp.dot(normed, wk_f32, preferred_element_type=jnp.float32).reshape(BATCH, SEQ_LEN, KV_HEADS, HEAD_DIM)
    keys_all = rotate(k_lin, cos_t[:, :, None], sin_t[:, :, None]).astype(jnp.bfloat16).astype(jnp.float32)
    values_all = jnp.dot(normed, wv_f32, preferred_element_type=jnp.float32).astype(jnp.bfloat16).astype(jnp.float32).reshape(BATCH, SEQ_LEN, KV_HEADS, HEAD_DIM)
    attn_flat = attention(queries, keys_all, values_all, seg_ids)
    proj_out = jnp.dot(attn_flat, wo_f32, preferred_element_type=jnp.float32).reshape(BATCH, SEQ_LEN, D_MODEL)
    return (hidden_f32 + proj_out).astype(jnp.bfloat16)


def reference(hidden, grad_out, positions, seg_ids, w_q, w_k, w_v, w_o, norm_gain):
    def run_block(hidden_in, wq_f32, wk_f32, wv_f32, wo_f32, gain_f32):
        return forward(hidden_in, positions, seg_ids, wq_f32, wk_f32, wv_f32, wo_f32, gain_f32)

    block_out, pullback = jax.vjp(run_block, hidden, w_q.astype(jnp.float32), w_k.astype(jnp.float32), w_v.astype(jnp.float32), w_o.astype(jnp.float32), norm_gain.astype(jnp.float32))
    grad_hidden, grad_wq, grad_wk, grad_wv, grad_wo, grad_gain = pullback(grad_out)
    return block_out, grad_hidden, grad_wq, grad_wk, grad_wv, grad_wo, grad_gain
```

```python
import functools

import jax
import jax.numpy as jnp
from jax import lax
from jax.experimental import pallas as pl
from jax.experimental.pallas import tpu as pltpu
from jax.sharding import PartitionSpec as P

HEAD_DIM = 128
NORM_EPS = 1e-5
ROPE_BASE = 500000.0
NEG_BIG = -1e30
LOG2E = 1.4426950408889634
N_DEV = 16
KEY_BLOCK = 256
ORDERS = ((2, 4, 8), (4, 8, 2), (8, 2, 4))
W_SIZES = (704, 704, 640)
WO_SIZES = (320, 320, 384)


NT = (((1,), (1,)), ((), ()))
NN = (((1,), (0,)), ((), ()))
TN = (((0,), (0,)), ((), ()))


def dot(a, b, dims):
    return lax.dot_general(a, b, dims, preferred_element_type=jnp.float32)


def swap(value, mask):
    return lax.ppermute(value, 'cp', [(i, i ^ mask) for i in range(N_DEV)])


def stack_heads(block, n_heads):
    return jnp.concatenate([block[:, h * HEAD_DIM:(h + 1) * HEAD_DIM] for h in range(n_heads)], axis=0)


def turn(x, cos_t, sin_t):
    return x * cos_t + pltpu.roll(x, HEAD_DIM // 2, 1) * sin_t


def allowed_keys(kb, qidx, start_row, n_rows):
    kidx = kb * KEY_BLOCK + lax.broadcasted_iota(jnp.int32, (KEY_BLOCK, n_rows), 0)
    return (kidx >= start_row) & (kidx <= qidx)


def query_index(glob, chunk, n_rows):
    lane = lax.broadcasted_iota(jnp.int32, (1, n_rows), 1)
    return glob * chunk + lane % chunk


def forward_kernel(glob_ref, low_ref, full_ref, q_ref, k_ref, v_ref, cos_ref, sin_ref, start_ref,
                   o_ref, qrot_ref, lse_ref, krot_ref, vglob_ref, vt_ref, acc_ref, max_ref, sum_ref, *, chunk, n_chunks, n_heads):
    step = pl.program_id(0)
    n_rows = n_heads * chunk
    to_log2 = HEAD_DIM ** -0.5 * LOG2E

    @pl.when(step == 0)
    def _():
        def place(i, _):
            src = pl.ds(pl.multiple_of(i * chunk, chunk), chunk)
            dst = pl.ds(pl.multiple_of(glob_ref[i] * chunk, chunk), chunk)
            krot_ref[dst, :] = turn(k_ref[src, :], cos_ref[src, :], sin_ref[src, :]).astype(jnp.bfloat16)
            vglob_ref[dst, :] = v_ref[src, :].astype(jnp.bfloat16)
            return 0
        lax.fori_loop(0, n_chunks, place, 0)
        for j in range(n_chunks * chunk // KEY_BLOCK):
            cols = slice(j * KEY_BLOCK, (j + 1) * KEY_BLOCK)
            vt_ref[:, cols] = vglob_ref[cols, :].astype(jnp.float32).T.astype(jnp.bfloat16)

    glob = glob_ref[step]
    rows = pl.ds(pl.multiple_of(step * chunk, chunk), chunk)
    cos_q, sin_q = cos_ref[rows, :], sin_ref[rows, :]
    for h in range(n_heads):
        cols = slice(h * HEAD_DIM, (h + 1) * HEAD_DIM)
        qrot_ref[:, cols] = turn(q_ref[:, cols], cos_q, sin_q).astype(jnp.bfloat16)
    queries = stack_heads(qrot_ref[...], n_heads)
    qidx = query_index(glob, chunk, n_rows)
    start_row = start_ref[0]

    def block(kb, masked, first):
        keys_at = pl.ds(pl.multiple_of(kb * KEY_BLOCK, KEY_BLOCK), KEY_BLOCK)
        scores = dot(krot_ref[keys_at, :], queries, NT)
        if masked:
            scores = jnp.where(allowed_keys(kb, qidx, start_row, n_rows), scores, NEG_BIG)
        top = jnp.max(scores, axis=0, keepdims=True)
        if not first:
            old = max_ref[...]
            top = jnp.maximum(top, old)
            decay = jnp.exp2((old - top) * to_log2)
        probs = jnp.exp2(scores * to_log2 - top * to_log2)
        total = jnp.sum(probs, axis=0, keepdims=True)
        out = dot(vt_ref[:, keys_at], probs.astype(jnp.bfloat16), NN)
        if not first:
            total = total + sum_ref[...] * decay
            out = out + acc_ref[...] * decay
        max_ref[...] = top
        sum_ref[...] = total
        acc_ref[...] = out

    last = (glob * chunk + chunk - 1) // KEY_BLOCK
    low, full = low_ref[step], jnp.minimum(full_ref[step], last)
    block(last, True, True)

    @pl.loop(low, full)
    def _(kb):
        block(kb, True, False)

    @pl.loop(jnp.maximum(low, full), last)
    def _(kb):
        block(kb, False, False)

    lse_ref[0] = max_ref[...] * to_log2 + jnp.log2(sum_ref[...])
    out = (acc_ref[...] / sum_ref[...]).T.astype(jnp.bfloat16)
    for h in range(n_heads):
        o_ref[:, h * HEAD_DIM:(h + 1) * HEAD_DIM] = out[h * chunk:(h + 1) * chunk]


def backward_kernel(glob_ref, low_ref, full_ref, q_ref, do_ref, o_ref, k_ref, v_ref, cos_ref, sin_ref, start_ref, lse_ref, dk_in, dv_in, dq_in,
                    out_ref, dk_ref, dv_ref, kv_ref, kt_ref, dq_ref, *, chunk, n_chunks, n_heads, base, count):
    step = pl.program_id(0)
    n_rows = n_heads * chunk
    scale = HEAD_DIM ** -0.5
    to_log2 = scale * LOG2E

    @pl.when(step == 0)
    def _():
        dk_ref[...] = dk_in[...]
        dv_ref[...] = dv_in[...]
        for j in range(n_chunks * chunk // KEY_BLOCK):
            cols = slice(j * KEY_BLOCK, (j + 1) * KEY_BLOCK)
            kt_ref[:, cols] = k_ref[cols, :].astype(jnp.float32).T.astype(jnp.bfloat16)

    slot = step + base
    glob = glob_ref[slot]
    queries = stack_heads(q_ref[...], n_heads)
    d_out = stack_heads(do_ref[...], n_heads)
    delta = jnp.sum((d_out.astype(jnp.float32) * stack_heads(o_ref[...], n_heads).astype(jnp.float32)).T, axis=0, keepdims=True)
    qidx = query_index(glob, chunk, n_rows)
    start_row = start_ref[0]
    lse = lse_ref[0]
    dq_ref[...] = jnp.zeros_like(dq_ref)

    def block(kb, masked):
        keys_at = pl.ds(pl.multiple_of(kb * KEY_BLOCK, KEY_BLOCK), KEY_BLOCK)
        scores = dot(k_ref[keys_at, :], queries, NT)
        if masked:
            scores = jnp.where(allowed_keys(kb, qidx, start_row, n_rows), scores, NEG_BIG)
        probs = jnp.exp2(scores * to_log2 - lse)
        d_probs = dot(v_ref[keys_at, :], d_out, NT)
        d_scores = (probs * (d_probs - delta)).astype(jnp.bfloat16)
        dv_ref[keys_at, :] += dot(probs.astype(jnp.bfloat16), d_out, NN)
        dk_ref[keys_at, :] += dot(d_scores, queries, NN)
        dq_ref[...] += dot(kt_ref[:, keys_at], d_scores, NN)

    last = (glob * chunk + chunk - 1) // KEY_BLOCK
    low, full = low_ref[slot], jnp.minimum(full_ref[slot], last)
    block(last, True)

    @pl.loop(low, full)
    def _(kb):
        block(kb, True)

    @pl.loop(jnp.maximum(low, full), last)
    def _(kb):
        block(kb, False)

    rows = pl.ds(pl.multiple_of(slot * chunk, chunk), chunk)
    cos_q, sin_q = cos_ref[rows, :], sin_ref[rows, :]
    dq = (dq_ref[...] * scale).T
    for h in range(n_heads):
        out_ref[:, h * HEAD_DIM:(h + 1) * HEAD_DIM] = turn(dq[h * chunk:(h + 1) * chunk], cos_q, -sin_q).astype(jnp.bfloat16)

    if base + count == n_chunks:
        @pl.when(step == count - 1)
        def _():
            def place(i, _):
                dst = pl.ds(pl.multiple_of(i * chunk, chunk), chunk)
                src = pl.ds(pl.multiple_of(glob_ref[i] * chunk, chunk), chunk)
                dk = turn(dk_ref[src, :] * scale, cos_ref[dst, :], -sin_ref[dst, :])
                kv_ref[dst, :HEAD_DIM] = dk.astype(jnp.bfloat16)
                kv_ref[dst, HEAD_DIM:] = dv_ref[src, :].astype(jnp.bfloat16)
                return 0
            lax.fori_loop(0, n_chunks, place, 0)


def attention_forward(qkv, cos_t, sin_t, start_rows, tables, chunk, n_chunks, n_heads):
    n_tok = chunk * n_chunks
    width = n_heads * HEAD_DIM
    n_rows = n_heads * chunk
    elems = n_tok * n_tok * n_heads * 9 // 16
    whole = lambda s: pl.BlockSpec(s, lambda i, *_: (0,) * len(s))
    grid_spec = pltpu.PrefetchScalarGridSpec(
        num_scalar_prefetch=3,
        grid=(n_chunks,),
        in_specs=[
            pl.BlockSpec((chunk, width), lambda i, *_: (i, 0)),
            pl.BlockSpec((n_tok, HEAD_DIM), lambda i, *_: (0, n_heads)),
            pl.BlockSpec((n_tok, HEAD_DIM), lambda i, *_: (0, n_heads + 1)),
            whole((n_tok, HEAD_DIM)),
            whole((n_tok, HEAD_DIM)),
            pl.BlockSpec((1, 1, n_rows), lambda i, *_: (i, 0, 0)),
        ],
        out_specs=[
            pl.BlockSpec((chunk, width), lambda i, *_: (i, 0)),
            pl.BlockSpec((chunk, width), lambda i, *_: (i, 0)),
            pl.BlockSpec((1, 1, n_rows), lambda i, *_: (i, 0, 0)),
            whole((n_tok, HEAD_DIM)),
            whole((n_tok, HEAD_DIM)),
        ],
        scratch_shapes=[
            pltpu.VMEM((HEAD_DIM, n_tok), jnp.bfloat16),
            pltpu.VMEM((HEAD_DIM, n_rows), jnp.float32),
            pltpu.VMEM((1, n_rows), jnp.float32),
            pltpu.VMEM((1, n_rows), jnp.float32),
        ],
    )
    return pl.pallas_call(
        functools.partial(forward_kernel, chunk=chunk, n_chunks=n_chunks, n_heads=n_heads),
        grid_spec=grid_spec,
        out_shape=[
            jax.ShapeDtypeStruct((n_tok, width), jnp.bfloat16),
            jax.ShapeDtypeStruct((n_tok, width), jnp.bfloat16),
            jax.ShapeDtypeStruct((n_chunks, 1, n_rows), jnp.float32),
            jax.ShapeDtypeStruct((n_tok, HEAD_DIM), jnp.bfloat16),
            jax.ShapeDtypeStruct((n_tok, HEAD_DIM), jnp.bfloat16),
        ],
        compiler_params=pltpu.CompilerParams(dimension_semantics=("arbitrary",), vmem_limit_bytes=40 << 20),
        cost_estimate=pl.CostEstimate(flops=4 * elems * HEAD_DIM, bytes_accessed=20 << 20, transcendentals=elems),
        name="attention_forward",
    )(*tables, qkv, qkv, qkv, cos_t, sin_t, start_rows)


def attention_backward(state, queries, d_out, out, keys, values, cos_t, sin_t, start_rows, lse, tables, chunk, n_chunks, n_heads, base, count):
    n_tok = chunk * n_chunks
    width = n_heads * HEAD_DIM
    n_rows = n_heads * chunk
    elems = n_tok * n_tok * n_heads * 9 // 16 * count // n_chunks
    whole = lambda s: pl.BlockSpec(s, lambda i, *_: (0,) * len(s))
    by_chunk = pl.BlockSpec((chunk, width), lambda i, *_: (i + base, 0))
    by_row = pl.BlockSpec((1, 1, n_rows), lambda i, *_: (i + base, 0, 0))
    tok = whole((n_tok, HEAD_DIM))
    d_query, d_key, d_value = state
    grid_spec = pltpu.PrefetchScalarGridSpec(
        num_scalar_prefetch=3,
        grid=(count,),
        in_specs=[by_chunk, by_chunk, by_chunk] + [tok] * 4 + [by_row, by_row, tok, tok, pl.BlockSpec(memory_space=pl.ANY)],
        out_specs=[by_chunk, tok, tok, whole((n_tok, 2 * HEAD_DIM))],
        scratch_shapes=[
            pltpu.VMEM((HEAD_DIM, n_tok), jnp.bfloat16),
            pltpu.VMEM((HEAD_DIM, n_rows), jnp.float32),
        ],
    )
    return pl.pallas_call(
        functools.partial(backward_kernel, chunk=chunk, n_chunks=n_chunks, n_heads=n_heads, base=base, count=count),
        grid_spec=grid_spec,
        out_shape=[
            jax.ShapeDtypeStruct((n_tok, width), jnp.bfloat16),
            jax.ShapeDtypeStruct((n_tok, HEAD_DIM), jnp.float32),
            jax.ShapeDtypeStruct((n_tok, HEAD_DIM), jnp.float32),
            jax.ShapeDtypeStruct((n_tok, 2 * HEAD_DIM), jnp.bfloat16),
        ],
        input_output_aliases={14: 0},
        compiler_params=pltpu.CompilerParams(dimension_semantics=("arbitrary",), vmem_limit_bytes=40 << 20),
        cost_estimate=pl.CostEstimate(flops=10 * elems * HEAD_DIM, bytes_accessed=24 << 20, transcendentals=elems),
        name=f"attention_backward_{base}",
    )(*tables, queries, d_out, out, keys, values, cos_t, sin_t, start_rows, lse, d_key, d_value, d_query)


def scatter_stages(matrix, rank, sizes):
    blocks = []
    base = 0
    for size in sizes:
        blocks.append(lax.slice_in_dim(matrix, base, base + size, axis=0))
        base += size
    for stage in range(3):
        sent = []
        for block, order in zip(blocks, ORDERS):
            length = block.shape[0] // 2
            bit = (rank // order[stage]) % 2
            give = lax.dynamic_slice_in_dim(block, (1 - bit) * length, length, axis=0)
            keep = lax.dynamic_slice_in_dim(block, bit * length, length, axis=0)
            sent.append((keep, swap(give, order[stage])))
        blocks = [keep + other for keep, other in sent]
        yield blocks


MESH_ID = pl.DeviceIdType.MESH


def flip(rank, mask):
    for bit in (1, 2, 4, 8):
        if mask & bit:
            rank = rank + bit * (1 - 2 * ((rank // bit) % 2))
    return rank


def gather_job(out_ref, part, src_ref, src_at, base, size, rank, core, sems):
    order = ORDERS[part]
    lengths = (size // 8, size // 4, size // 2)
    bits = [(rank // mask) % 2 for mask in order]
    own = base + bits[0] * (size // 2) + bits[1] * (size // 4) + bits[2] * (size // 8)
    offsets = (own, base + bits[0] * (size // 2) + bits[1] * (size // 4), base + bits[0] * (size // 2))
    send, recv, d2d_send, d2d_recv, local = sems
    rows = lambda off, n: pl.ds(pl.multiple_of(off, 8), n)

    def remote(src, dst, a, b, mask):
        return pltpu.make_async_remote_copy(src_ref=src, dst_ref=dst, send_sem=a, recv_sem=b, device_id=(flip(rank, mask),), device_id_type=MESH_ID)

    def hop(s):
        spot = out_ref.at[core, rows(offsets[s], lengths[s])]
        src = src_ref.at[src_at(lengths[0])] if s == 0 else spot
        return remote(src, spot, send.at[s], recv.at[s], order[2 - s])

    def cross(s):
        if s == 0:
            src = src_ref.at[src_at(lengths[0])]
            spot = out_ref.at[core, rows(own, lengths[0])]
        else:
            off = offsets[s - 1] + (1 - 2 * bits[3 - s]) * lengths[s - 1]
            spot = out_ref.at[core, rows(off, lengths[s - 1])]
            src = spot
        return remote(src, spot, d2d_send.at[s], d2d_recv.at[s], 1)

    keep = pltpu.make_async_copy(src_ref.at[src_at(lengths[0])], out_ref.at[core, rows(own, lengths[0])], local)
    hops = [hop(s) for s in range(3)]
    crosses = [cross(s) for s in range(4)]

    def first():
        hops[0].start()
        crosses[0].start()
        keep.start()

    def second():
        keep.wait()
        hops[0].wait_recv()
        hops[1].start()
        crosses[1].start()

    def third():
        hops[1].wait_recv()
        hops[2].start()
        crosses[2].start()

    def fourth():
        hops[2].wait_recv()
        crosses[3].start()

    def drain():
        for copy in hops:
            copy.wait_send()
        for copy in crosses:
            copy.wait()

    return first, second, third, fourth, drain


def tail_kernel(dw_ref, wo0_ref, wo1_ref, wo2_ref, gh_ref, gain_ref, gw_ref, gwo_ref, gh_out, gain_out,
                keep0, keep1, keep2, recv0, recv1, recv2, slots, rs_send, rs_recv, load_sem,
                ag_send, ag_recv, d2d_send, d2d_recv, local_sem, gh_send, gh_recv, gh_local, gain_send, gain_recv, *, sizes, wo_sizes):
    rank = lax.axis_index('cp')
    chip, core = rank // 2, rank % 2
    barrier = pltpu.get_barrier_semaphore()
    for mask in range(1, N_DEV):
        pl.semaphore_signal(barrier, inc=1, device_id=(flip(rank, mask),), device_id_type=MESH_ID)
    pl.semaphore_wait(barrier, N_DEV - 1)

    def remote(src, dst, a, b, mask):
        return pltpu.make_async_remote_copy(src_ref=src, dst_ref=dst, send_sem=a, recv_sem=b, device_id=(flip(rank, mask),), device_id_type=MESH_ID)

    keeps, recvs = (keep0, keep1, keep2), (recv0, recv1, recv2)
    rows = lambda off, n: pl.ds(pl.multiple_of(off, 8), n)
    scatter, loads, bases = [], [], []
    base = 0
    for part, size in enumerate(sizes):
        order = ORDERS[part]
        bits = [(rank // mask) % 2 for mask in order]
        half, quarter, eighth = size // 2, size // 4, size // 8
        keep, recv = keeps[part], recvs[part]
        loads.append(pltpu.make_async_copy(dw_ref.at[rows(base + bits[0] * half, half)], keep, load_sem.at[part]))
        at2, at3 = bits[1] * quarter, bits[1] * quarter + bits[2] * eighth
        scatter.append((
            remote(dw_ref.at[rows(base + (1 - bits[0]) * half, half)], recv.at[pl.ds(0, half)], rs_send.at[part, 0], rs_recv.at[part, 0], order[0]),
            remote(keep.at[rows((1 - bits[1]) * quarter, quarter)], recv.at[pl.ds(half, quarter)], rs_send.at[part, 1], rs_recv.at[part, 1], order[1]),
            remote(keep.at[rows(at2 + (1 - bits[2]) * eighth, eighth)], recv.at[pl.ds(half + quarter, eighth)], rs_send.at[part, 2], rs_recv.at[part, 2], order[2]),
            ((0, half, 0), (at2, quarter, half), (at3, eighth, half + quarter)),
        ))
        bases.append((base, at3))
        base += size

    for part in range(3):
        scatter[part][0].start()
    for load in loads:
        load.start()
    wo_jobs, wo_base = [], 0
    for part, (size, shard) in enumerate(zip(wo_sizes, (wo0_ref, wo1_ref, wo2_ref))):
        sems = (ag_send.at[3 + part], ag_recv.at[3 + part], d2d_send.at[3 + part], d2d_recv.at[3 + part], local_sem.at[3 + part])
        wo_jobs.append(gather_job(gwo_ref, part, shard, lambda n: pl.ds(0, n), wo_base, size, rank, core, sems))
        wo_base += size
    jobs = []
    for part, size in enumerate(sizes):
        sems = (ag_send.at[part], ag_recv.at[part], d2d_send.at[part], d2d_recv.at[part], local_sem.at[part])
        at3 = bases[part][1]
        jobs.append(gather_job(gw_ref, part, keeps[part], lambda n, at=at3: rows(at, n), bases[part][0], size, rank, core, sems))

    for job in wo_jobs:
        job[0]()
    moves = [remote(gh_ref.at[m], gh_out.at[chip], gh_send.at[m], gh_recv.at[m], 2 * m) for m in range(1, N_DEV // 2)]
    for move in moves:
        move.start()
    stay = pltpu.make_async_copy(gh_ref.at[0], gh_out.at[chip], gh_local)
    stay.start()
    gains = [remote(gain_ref, slots.at[mask], gain_send.at[mask], gain_recv.at[mask], mask) for mask in range(1, N_DEV)]
    for gain in gains:
        gain.start()

    def add_stage(part, stage):
        at, count, src = scatter[part][3][stage]
        scatter[part][stage].wait_recv()
        keep, recv = keeps[part], recvs[part]
        n_tiles = count // 8

        @pl.loop(0, n_tiles)
        def _(t):
            here = pl.ds(pl.multiple_of(at + t * 8, 8), 8)
            there = pl.ds(pl.multiple_of(src + t * 8, 8), 8)
            keep[here, :] += recv[there, :]

    for load in loads:
        load.wait()
    for stage in range(3):
        for part in range(3):
            add_stage(part, stage)
            if stage < 2:
                scatter[part][stage + 1].start()
            else:
                jobs[part][0]()
        for job in wo_jobs:
            job[stage + 1]()
    for step in range(1, 4):
        for job in jobs:
            job[step]()

    for gain in gains:
        gain.wait()
    total = gain_ref[...]
    slots[0] = total
    level = [slots[i] for i in range(N_DEV)]
    while len(level) > 1:
        level = [level[2 * i] + level[2 * i + 1] for i in range(len(level) // 2)]
    gain_out[...] = level[0]
    for part in range(3):
        for stage in range(3):
            scatter[part][stage].wait_send()
    for job in jobs + wo_jobs:
        job[4]()
    for move in moves:
        move.wait()
    stay.wait()


def exchange_tail(d_w, wo_shards, grad_pieces, gain, sizes, wo_sizes):
    cols = d_w.shape[1]
    wo_cols = wo_shards[0].shape[1]
    any_spec = pl.BlockSpec(memory_space=pl.ANY)
    vmem = pl.BlockSpec(memory_space=pltpu.VMEM)
    dma = pltpu.SemaphoreType.DMA
    keeps = [pltpu.VMEM((size // 2, cols), jnp.float32) for size in sizes]
    recvs = [pltpu.VMEM((size // 2 + size // 4 + size // 8, cols), jnp.float32) for size in sizes]
    return pl.pallas_call(
        functools.partial(tail_kernel, sizes=sizes, wo_sizes=wo_sizes),
        in_specs=[any_spec] * 5 + [vmem],
        out_specs=[any_spec, any_spec, any_spec, vmem],
        out_shape=[
            jax.ShapeDtypeStruct((2, sum(sizes), cols), jnp.float32),
            jax.ShapeDtypeStruct((2, sum(wo_sizes), wo_cols), jnp.float32),
            jax.ShapeDtypeStruct(grad_pieces.shape, grad_pieces.dtype),
            jax.ShapeDtypeStruct(gain.shape, jnp.float32),
        ],
        scratch_shapes=keeps + recvs + [
            pltpu.VMEM((N_DEV,) + gain.shape, jnp.float32),
            dma((3, 3)), dma((3, 3)), dma((3,)),
            dma((6, 3)), dma((6, 3)), dma((6, 4)), dma((6, 4)), dma((6,)),
            dma((8,)), dma((8,)), dma, dma((N_DEV,)), dma((N_DEV,)),
        ],
        compiler_params=pltpu.CompilerParams(collective_id=0, has_side_effects=True, vmem_limit_bytes=56 << 20),
        name="exchange_tail",
    )(d_w, *wo_shards, grad_pieces, gain)


def solution(mesh):
    def local_step(hidden, grad_out, positions, seg_ids, w_q, w_k, w_v, w_o, norm_gain):
        n_rows, n_tok, d_model = hidden.shape
        chunk = n_tok // 2
        n_chunks = 2 * N_DEV
        seq = N_DEV * n_tok
        half_tok = seq // 2
        width = w_q.shape[1] // 2
        n_heads = width // HEAD_DIM
        rank = lax.axis_index('cp')
        chip, core = rank // 2, rank % 2

        def to_rows(array):
            pieces = []
            for m in range(n_rows):
                piece = lax.dynamic_index_in_dim(array, jnp.bitwise_xor(chip, m), axis=0, keepdims=True)
                pieces.append(piece if m == 0 else swap(piece, 2 * m))
            return jnp.concatenate(pieces, axis=0)

        def from_rows(array):
            result = jnp.zeros_like(array)
            for m in range(n_rows):
                piece = array[m:m + 1]
                piece = piece if m == 0 else swap(piece, 2 * m)
                result = lax.dynamic_update_slice_in_dim(result, piece, jnp.bitwise_xor(chip, m), axis=0)
            return result

        pos_own = to_rows(positions)
        pos_all = jnp.concatenate([pos_own, swap(pos_own, 1)], axis=0)
        x_own = to_rows(hidden).reshape(half_tok, d_model)
        dy_own = to_rows(grad_out).reshape(half_tok, d_model)

        slots = jnp.arange(n_chunks)
        owner = jnp.bitwise_xor(rank, jnp.bitwise_xor(slots // 16, (slots // 2) % 8 * 2))
        glob = jnp.where(slots % 2 == 0, owner, n_chunks - 1 - owner).astype(jnp.int32)
        pos_chunk = pos_all.reshape(n_chunks, chunk)
        start = glob[:, None] * chunk + jnp.arange(chunk)[None, :] - pos_chunk
        start_rows = jnp.tile(start, (1, n_heads))[:, None, :].astype(jnp.int32)
        tables = (glob, (start[:, 0] // KEY_BLOCK).astype(jnp.int32), ((start[:, -1] + KEY_BLOCK - 1) // KEY_BLOCK).astype(jnp.int32))
        inv_freq = ROPE_BASE ** (-jnp.arange(0, HEAD_DIM, 2).astype(jnp.float32) / HEAD_DIM)
        angles = pos_all.reshape(-1).astype(jnp.float32)[:, None] * inv_freq
        cos_h, sin_h = jnp.cos(angles), jnp.sin(angles)
        cos_t = jnp.concatenate([cos_h, cos_h], axis=-1)
        sin_t = jnp.concatenate([-sin_h, sin_h], axis=-1)

        def head_cols(w, which):
            size = w.shape[1] // 2
            return lax.dynamic_slice_in_dim(w, which * size, size, axis=1)

        w_own = jnp.concatenate([head_cols(w, core) for w in (w_q, w_k, w_v)], axis=1)
        w_par = jnp.concatenate([head_cols(w, 1 - core) for w in (w_q, w_k, w_v)], axis=1)
        wo_own = lax.dynamic_slice_in_dim(w_o, core * width, width, axis=0)
        wo_par = lax.dynamic_slice_in_dim(w_o, (1 - core) * width, width, axis=0)
        gain = norm_gain.astype(jnp.float32)

        x_f32 = x_own.astype(jnp.float32)
        inv_rms = lax.rsqrt(jnp.mean(x_f32 * x_f32, axis=-1, keepdims=True) + NORM_EPS)
        h_own = (x_f32 * inv_rms * gain).astype(jnp.bfloat16)
        h_all = jnp.concatenate([h_own, swap(h_own, 1)], axis=0)
        qkv = dot(h_all, w_own, NN)
        attn, queries, lse, keys, values = attention_forward(qkv, cos_t, sin_t, start_rows, tables, chunk, n_chunks, n_heads)

        dy_all = jnp.concatenate([dy_own, swap(dy_own, 1)], axis=0)
        d_attn = dot(dy_all, wo_own, NT).astype(jnp.bfloat16)
        d_wo = dot(attn, dy_all, TN)
        attn_par = swap(attn[half_tok:], 1)
        proj = dot(jnp.concatenate([attn[:half_tok], attn_par], axis=1), jnp.concatenate([wo_own, wo_par], axis=0), NN)
        out_own = (x_f32 + proj).astype(jnp.bfloat16)
        block_out = from_rows(out_own.reshape(n_rows, n_tok, d_model))

        state = (jnp.zeros((seq, width), jnp.bfloat16), jnp.zeros((seq, HEAD_DIM), jnp.float32), jnp.zeros((seq, HEAD_DIM), jnp.float32))
        stages = scatter_stages(d_wo, rank, WO_SIZES)
        count = n_chunks // 4
        for call in range(4):
            if call:
                if call > 1:
                    shards = next(stages)
                    state, shards[:] = lax.optimization_barrier((state, shards))
            *state, d_kv = attention_backward(state, queries, d_attn, attn, keys, values, cos_t, sin_t, start_rows, lse, tables, chunk, n_chunks, n_heads, call * count, count)
        shards = next(stages)
        d_qkv = jnp.concatenate([state[0], d_kv], axis=1)
        d_w = dot(h_all, d_qkv, TN)
        d_qkv_par = swap(d_qkv[half_tok:], 1)
        d_normed = dot(jnp.concatenate([d_qkv[:half_tok], d_qkv_par], axis=1), jnp.concatenate([w_own, w_par], axis=1), NT)
        d_normed = d_normed.astype(jnp.bfloat16).astype(jnp.float32)
        x_hat = x_f32 * inv_rms
        d_hat = d_normed * gain
        d_hidden = inv_rms * (d_hat - x_hat * jnp.mean(d_hat * x_hat, axis=-1, keepdims=True))
        grad_own = (dy_own.astype(jnp.float32) + d_hidden).astype(jnp.bfloat16)
        gain_part = jnp.sum(d_normed * x_hat, axis=0)
        pieces = grad_own.reshape(n_rows, n_tok, d_model)
        gw, gwo, grad_hidden, grad_gain = exchange_tail(d_w, shards, pieces, gain_part.reshape(8, d_model // 8), W_SIZES, WO_SIZES)
        grad_wq = jnp.concatenate([gw[0, :, :width], gw[1, :, :width]], axis=1)
        grad_wk = jnp.concatenate([gw[0, :, width:width + HEAD_DIM], gw[1, :, width:width + HEAD_DIM]], axis=1)
        grad_wv = jnp.concatenate([gw[0, :, width + HEAD_DIM:], gw[1, :, width + HEAD_DIM:]], axis=1)
        return block_out, grad_hidden, grad_wq, grad_wk, grad_wv, gwo.reshape(w_o.shape), grad_gain.reshape(d_model)

    seq_spec = P(None, 'cp', None)
    tok_spec = P(None, 'cp')
    full_spec = P()
    return jax.shard_map(local_step, mesh=mesh, in_specs=(seq_spec, seq_spec, tok_spec, tok_spec, full_spec, full_spec, full_spec, full_spec, full_spec), out_specs=(seq_spec, seq_spec, full_spec, full_spec, full_spec, full_spec, full_spec), check_vma=False)
```
